512 devices in a mesh: spec: 64 (over x_hi, z, core), img: 8 (over x_lo, y).
Axes of the slice: x: 4 (x_hi: 2, x_lo: 2; x = x_hi * 2 + x_lo), y: 4, z: 16, core: 2. Of those that a mesh axis runs over, the one named last changes fastest.
Arguments:
- spec_emb: bfloat16 [8192, 1024], P('spec', 'img'), may hold values from -1024 to 1024
- img_emb: bfloat16 [2048, 1024], P('img', 'spec'), may hold values from -16 to 16
- grad_spec: bfloat16 [8192, 1024], P('spec', 'img'), may hold values from -6 to 6
- grad_img: bfloat16 [2048, 1024], P('img', 'spec'), may hold values from -6 to 6
Outputs:
- spec_emb_grad: bfloat16 [8192, 1024], P('spec', 'img')
- img_emb_grad: bfloat16 [2048, 1024], P('img', 'spec')
The draws below stay inside these ranges and needn't reach their ends.
All inputs are finite; a program needn't handle non-finite values.
Results may differ from the reference program's by a relative error of at most 0.0109.
Values may be sent and summed in bfloat16 or wider, within the bound.
No kernel may reach another device: no remote copies, remote signals or barrier semaphores. Data moves between devices by JAX's collectives and lax.ppermute only.
A program may use at most 64 MiB of HBM per device.

```python
import jax
import jax.numpy as jnp
from jax import lax

D = 1024
HEADS = 16
SPEC = 8192
IMG = 2048


def drawn_pair(key):
    base = jax.random.fold_in(key, 4111)
    streams = jax.random.split(base, 2)
    image_rows = jax.random.truncated_normal(streams[0], -6.0, 6.0, (IMG, D), jnp.float32)
    spec_rows = jax.random.truncated_normal(streams[1], -6.0, 6.0, (SPEC, D), jnp.float32)
    return (spec_rows, image_rows)


def draw_spec_emb(key, part):
    return drawn_pair(key)[0].astype(jnp.bfloat16)


def draw_img_emb(key, part):
    return drawn_pair(key)[1].astype(jnp.bfloat16)


def levels(key, extent, cuts, low, high):
    level = 1.0
    for dim, shards_of in cuts:
        heights = jax.random.uniform(jax.random.fold_in(jax.random.fold_in(key, 6), dim), (shards_of,), jnp.float32, low / len(cuts), high / len(cuts))
        level = level * jnp.repeat(jnp.exp(heights), extent[dim] // shards_of).reshape((-1,) + (1,) * (len(extent) - 1 - dim))
    return level


def scatter_about(own_key, extent, spread, most, cuts=(), dtype=jnp.bfloat16):
    level = levels(own_key, extent, cuts, -0.22, 0.18) if cuts else 1.0
    drawn = jax.random.normal(own_key, extent, jnp.float32) * spread * level
    return jnp.minimum(jnp.maximum(drawn, -most), most).astype(dtype)


def setup_inputs(seed: int = 0) -> dict:
    key_list = jax.random.split(jax.random.key(seed), 5)
    return {
        "spec_emb": draw_spec_emb(jax.random.fold_in(key_list[4], 71), 0),
        "img_emb": draw_img_emb(jax.random.fold_in(key_list[4], 71), 0),
        "grad_spec": scatter_about(key_list[2], (SPEC, D), 1.0, 6.0, ((0, 64), (1, 8))),
        "grad_img": scatter_about(key_list[3], (IMG, D), 1.0, 6.0, ((0, 8), (1, 64))),
    }


def head_terms(operands):
    spec_rows, spec_grad, image_rows, image_grad = operands
    scale = (D // HEADS) ** -0.5
    scores = jnp.dot(spec_rows, image_rows.T, preferred_element_type=jnp.float32) * scale
    row_moment = jnp.dot(spec_grad, image_rows.T, preferred_element_type=jnp.float32)
    column_moment = jnp.dot(spec_rows, image_grad.T, preferred_element_type=jnp.float32)
    row_scaled = jnp.exp(scores - jnp.max(scores, axis=1, keepdims=True))
    row_weight = row_scaled / jnp.sum(row_scaled, axis=1, keepdims=True)
    column_scaled = jnp.exp(scores - jnp.max(scores, axis=0, keepdims=True))
    column_weight = column_scaled / jnp.sum(column_scaled, axis=0, keepdims=True)
    row_delta = jnp.sum(row_weight * row_moment, axis=1, keepdims=True)
    column_delta = jnp.sum(column_weight * column_moment, axis=0, keepdims=True)
    slope = (row_weight * (row_moment - row_delta) + column_weight * (column_moment - column_delta)).astype(jnp.bfloat16)
    spec_part = scale * jnp.dot(slope, image_rows, preferred_element_type=jnp.float32) + jnp.dot(column_weight.astype(jnp.bfloat16), image_grad, preferred_element_type=jnp.float32)
    image_part = scale * jnp.dot(slope.T, spec_rows, preferred_element_type=jnp.float32) + jnp.dot(row_weight.astype(jnp.bfloat16).T, spec_grad, preferred_element_type=jnp.float32)
    return spec_part, image_part


def by_heads(array):
    return jnp.transpose(array.reshape(array.shape[0], HEADS, D // HEADS), (1, 0, 2))


def joined(array):
    return jnp.transpose(array, (1, 0, 2)).reshape(array.shape[1], D)


def reference(spec_emb, img_emb, grad_spec, grad_img):
    spec_parts, image_parts = lax.map(head_terms, (by_heads(spec_emb), by_heads(grad_spec), by_heads(img_emb), by_heads(grad_img)))
    return joined(spec_parts).astype(jnp.bfloat16), joined(image_parts).astype(jnp.bfloat16)
```

```python
import jax
import jax.numpy as jnp
from jax import lax
from jax.sharding import Mesh
from jax.sharding import PartitionSpec as P

D = 1024
HEADS = 16
SIZE = D // HEADS
SPEC = ("xh", "z3", "z2", "z1", "z0", "co")
IMG = ("xl", "y1", "y0")
EVERY = SPEC + IMG
GROUP = ("z0", "co", "xl", "y1", "y0")
ROWS = ("z0", "xl", "y1", "y0")
SCALE = SIZE**-0.5


def head_moves():
    pairs = []
    for source in range(512):
        xh, z3, z2, z1, z0, co, xl, y1, y0 = ((source >> k) & 1 for k in range(8, -1, -1))
        target = 0
        for bit in (xl, y1, y0, co, z0, z1, xh, 1 - z3, 1 - z2):
            target = 2 * target + bit
        pairs.append((source, target))
    return pairs


def dot(a, b, dims):
    return lax.dot_general(a, b, (dims, ((), ())), preferred_element_type=jnp.float32)


def moments(scores, moment, dim):
    highest = jnp.max(scores, axis=dim, keepdims=True)
    scaled = jnp.exp(scores - highest)
    return jnp.stack(
        (
            highest.reshape(-1),
            jnp.sum(scaled, axis=dim),
            jnp.sum(scaled * moment, axis=dim),
        )
    )


def totals(parts):
    highest = jnp.max(parts[:, 0], axis=0)
    factor = jnp.exp(parts[:, 0] - highest)
    total = jnp.sum(parts[:, 1] * factor, axis=0)
    return highest, total, jnp.sum(parts[:, 2] * factor, axis=0) / total


def shards(spec_emb, img_emb, grad_spec, grad_img):
    moves = head_moves()
    tokens = img_emb.shape[0]
    half = tokens // 2
    rows = spec_emb.shape[0]
    by_head = jnp.stack(
        [
            jnp.concatenate([a[:, h * SIZE : (h + 1) * SIZE] for a in (spec_emb, grad_spec)], axis=1)
            for h in range(2)
        ]
    )
    own = lax.all_to_all(by_head, "co", 0, 0, tiled=True).reshape(2 * rows, 2 * SIZE)
    own = lax.ppermute(own, EVERY, moves)
    features = 2 * img_emb.shape[1]
    image = jnp.concatenate([img_emb, grad_img], axis=1).T.reshape(features, 2, half)
    image = jnp.moveaxis(image, 1, 0)[None, :, None]
    image = jnp.broadcast_to(image, (2, 2, 8, features, half)).reshape(32, features, half)
    image = lax.all_to_all(image, GROUP, 0, 0, tiled=True)
    image = image.reshape(4, 8, 2, features // 2, half).transpose(2, 0, 3, 1, 4).reshape(2, SIZE, 8 * half)
    image_rows, image_grad = image[0], image[1]
    both = lax.all_gather(own, "co", tiled=True)
    spec_rows, spec_grad = both[:, :SIZE], both[:, SIZE:]

    across = ((1,), (0,))
    scores = dot(spec_rows, image_rows, across) * SCALE
    row_moment = dot(spec_grad, image_rows, across)
    column_moment = dot(spec_rows, image_grad, across)
    column_part = moments(scores, column_moment, 0)
    row_part = moments(scores, row_moment, 1)
    column_parts = lax.all_to_all(
        jnp.broadcast_to(column_part, (16, *column_part.shape)), ROWS, 0, 0, tiled=True
    )
    row_parts = lax.all_gather(row_part, "co")
    row_high, row_total, row_delta = (t[:, None] for t in totals(row_parts))
    column_high, column_total, column_delta = (t[None, :] for t in totals(column_parts))
    row_weight = jnp.exp(scores - row_high) / row_total
    column_weight = jnp.exp(scores - column_high) / column_total
    slope = (
        row_weight * (row_moment - row_delta) + column_weight * (column_moment - column_delta)
    ).astype(jnp.bfloat16)
    row_weight = row_weight.astype(jnp.bfloat16)
    column_weight = column_weight.astype(jnp.bfloat16)
    last = ((1,), (1,))
    spec_part = SCALE * dot(image_rows, slope, last) + dot(image_grad, column_weight, last)
    first = ((0,), (0,))
    image_part = SCALE * dot(spec_rows, slope, first) + dot(spec_grad, row_weight, first)

    spec_part = spec_part.astype(jnp.bfloat16).reshape(SIZE, 2, 2 * rows)
    spec_parts = lax.all_to_all(jnp.moveaxis(spec_part, 1, 0), "co", 0, 0, tiled=True)
    spec_sum = jnp.sum(spec_parts.astype(jnp.float32), axis=0).astype(jnp.bfloat16)
    spec_back = lax.ppermute(spec_sum, EVERY, [(b, a) for a, b in moves])

    image_part = image_part.astype(jnp.bfloat16).reshape(4, SIZE // 4, 8, half)
    image_part = jnp.moveaxis(image_part, 2, 1).reshape(32, SIZE // 4, half)
    image_parts = lax.all_to_all(image_part, GROUP, 0, 0, tiled=True)
    image_parts = image_parts.reshape(2, 2, 8, SIZE // 4, half).astype(jnp.float32)
    image_sum = jnp.sum(image_parts, axis=(0, 2)).astype(jnp.bfloat16)
    image_result = jnp.moveaxis(image_sum, 1, 2).reshape(tokens, SIZE // 4)

    spec_back = jnp.moveaxis(spec_back.reshape(SIZE, 2, rows), 1, 0)
    spec_heads = lax.all_to_all(spec_back, "co", 0, 0, tiled=True)
    spec_result = spec_heads.reshape(2 * SIZE, rows).T
    return (spec_result, image_result)


def solution(mesh):
    split = Mesh(mesh.devices.reshape((2,) * 9), EVERY)
    return jax.shard_map(
        shards,
        mesh=split,
        in_specs=(P(SPEC, IMG), P(IMG, SPEC), P(SPEC, IMG), P(IMG, SPEC)),
        out_specs=(P(SPEC, IMG), P(IMG, SPEC)),
        check_vma=False,
    )
```

```python
import jax
import jax.numpy as jnp
from jax import lax
from jax.sharding import Mesh
from jax.sharding import PartitionSpec as P


D = 1024
HEADS = 16
SIZE = D // HEADS
SPEC = ("xh", "z3", "z2", "z1", "z0", "co")
IMG = ("xl", "y1", "y0")
EVERY = SPEC + IMG
GROUP = ("z0", "co", "xl", "y1", "y0")
ROWS = ("z0", "xl", "y1", "y0")
SCALE = SIZE**-0.5


def head_moves():
    pairs = []
    for source in range(512):
        xh, z3, z2, z1, z0, co, xl, y1, y0 = ((source >> k) & 1 for k in range(8, -1, -1))
        target = 0
        for bit in (xl, y1, y0, co, z0, z1, xh, 1 - z3, 1 - z2):
            target = 2 * target + bit
        pairs.append((source, target))
    return pairs


def dot(a, b, dims):
    return lax.dot_general(a, b, (dims, ((), ())), preferred_element_type=jnp.float32)


def moments(scores, moment, dim):
    highest = jnp.max(scores, axis=dim, keepdims=True)
    scaled = jnp.exp(scores - highest)
    return jnp.stack(
        (
            highest.reshape(-1),
            jnp.sum(scaled, axis=dim),
            jnp.sum(scaled * moment, axis=dim),
        )
    )


def totals(parts):
    highest = jnp.max(parts[:, 0], axis=0)
    factor = jnp.exp(parts[:, 0] - highest)
    total = jnp.sum(parts[:, 1] * factor, axis=0)
    return highest, total, jnp.sum(parts[:, 2] * factor, axis=0) / total


def shards(spec_emb, img_emb, grad_spec, grad_img):
    moves = head_moves()
    tokens = img_emb.shape[0]
    half = tokens // 2
    rows = spec_emb.shape[0]
    second = lax.axis_index("co") == 1
    own = lax.all_gather(jnp.concatenate([spec_emb, grad_spec], axis=1), "co", tiled=True)
    own = jnp.concatenate(
        [jnp.where(second, a[:, SIZE:], a[:, :SIZE]) for a in (own[:, : 2 * SIZE], own[:, 2 * SIZE :])],
        axis=1,
    )
    own = lax.ppermute(own, EVERY, moves)
    features = 2 * img_emb.shape[1]
    image = jnp.concatenate([img_emb, grad_img], axis=1).T.reshape(features, 2, half)
    image = jnp.moveaxis(image, 1, 0)[None, :, None]
    image = jnp.broadcast_to(image, (2, 2, 8, features, half)).reshape(32, features, half)
    image = lax.all_to_all(image, GROUP, 0, 0, tiled=True)
    image = image.reshape(4, 8, 2, features // 2, half).transpose(2, 0, 3, 1, 4).reshape(2, SIZE, 8 * half)
    image_rows, image_grad = image[0], image[1]
    both = lax.all_gather(own, "co", tiled=True)
    spec_rows, spec_grad = both[:, :SIZE], both[:, SIZE:]

    across = ((1,), (0,))
    scores = dot(spec_rows, image_rows, across) * SCALE
    row_moment = dot(spec_grad, image_rows, across)
    column_moment = dot(spec_rows, image_grad, across)
    column_part = moments(scores, column_moment, 0)
    row_part = moments(scores, row_moment, 1)
    column_parts = lax.all_to_all(
        jnp.broadcast_to(column_part, (16, *column_part.shape)), ROWS, 0, 0, tiled=True
    )
    row_parts = lax.all_gather(row_part, "co")
    row_high, row_total, row_delta = (t[:, None] for t in totals(row_parts))
    column_high, column_total, column_delta = (t[None, :] for t in totals(column_parts))
    row_weight = jnp.exp(scores - row_high) / row_total
    column_weight = jnp.exp(scores - column_high) / column_total
    slope = (
        row_weight * (row_moment - row_delta) + column_weight * (column_moment - column_delta)
    ).astype(jnp.bfloat16)
    row_weight = row_weight.astype(jnp.bfloat16)
    column_weight = column_weight.astype(jnp.bfloat16)
    last = ((1,), (1,))
    spec_part = SCALE * dot(image_rows, slope, last) + dot(image_grad, column_weight, last)
    first = ((0,), (0,))
    image_part = SCALE * dot(spec_rows, slope, first) + dot(spec_grad, row_weight, first)

    spec_parts = lax.all_gather(spec_part.astype(jnp.bfloat16), "co")
    spec_parts = jnp.where(second, spec_parts[:, :, 2 * rows :], spec_parts[:, :, : 2 * rows])
    spec_sum = (spec_parts[0].astype(jnp.float32) + spec_parts[1]).astype(jnp.bfloat16)
    spec_back = lax.ppermute(spec_sum, EVERY, [(b, a) for a, b in moves])

    image_part = image_part.astype(jnp.bfloat16).reshape(4, SIZE // 4, 8, half)
    image_part = jnp.moveaxis(image_part, 2, 1).reshape(32, SIZE // 4, half)
    image_parts = lax.all_to_all(image_part, GROUP, 0, 0, tiled=True)
    image_parts = image_parts.reshape(2, 2, 8, SIZE // 4, half).astype(jnp.float32)
    image_sum = jnp.sum(image_parts, axis=(0, 2)).astype(jnp.bfloat16)
    image_result = jnp.moveaxis(image_sum, 1, 2).reshape(tokens, SIZE // 4)

    spec_heads = lax.all_gather(spec_back, "co", tiled=True)
    spec_result = jnp.where(second, spec_heads[:, rows:], spec_heads[:, :rows]).T
    return (spec_result, image_result)


def solution(mesh):
    split = Mesh(mesh.devices.reshape((2,) * 9), EVERY)

    return jax.shard_map(
        shards,
        mesh=split,
        in_specs=(P(SPEC, IMG), P(IMG, SPEC), P(SPEC, IMG), P(IMG, SPEC)),
        out_specs=(P(SPEC, IMG), P(IMG, SPEC)),
        check_vma=False,
    )
```

```python
import jax
import jax.numpy as jnp
from jax import lax
from jax.sharding import Mesh
from jax.sharding import PartitionSpec as P


D = 1024
HEADS = 16
SIZE = D // HEADS
SPEC = ("xh", "z3", "z2", "z1", "z0", "co")
IMG = ("xl", "y1", "y0")
EVERY = SPEC + IMG
GROUP = ("z0", "co", "xl", "y1", "y0")
ROWS = ("z0", "xl", "y1", "y0")
SCALE = SIZE**-0.5


def head_moves():
    pairs = []
    for source in range(512):
        xh, z3, z2, z1, z0, co, xl, y1, y0 = ((source >> k) & 1 for k in range(8, -1, -1))
        target = 0
        for bit in (xl, y1, y0, co, z0 ^ z1 ^ co ^ 1, z1, xh, 1 - z3, 1 - z2):
            target = 2 * target + bit
        pairs.append((source, target))
    return pairs


def dot(a, b, dims):
    return lax.dot_general(a, b, (dims, ((), ())), preferred_element_type=jnp.float32)


def moments(scores, moment, dim):
    highest = jnp.max(scores, axis=dim, keepdims=True)
    scaled = jnp.exp(scores - highest)
    sums = (jnp.sum(scaled, axis=dim), jnp.sum(scaled * moment, axis=dim))
    return jnp.stack((highest.reshape(-1), *sums)), scaled


def totals(parts, own):
    highest = jnp.max(parts[:, 0], axis=0)
    factor = jnp.exp(parts[:, 0] - highest)
    total = jnp.sum(parts[:, 1] * factor, axis=0)
    delta = jnp.sum(parts[:, 2] * factor, axis=0) / total
    return jnp.exp(own[0] - highest) / total, delta


def shards(spec_emb, img_emb, grad_spec, grad_img):
    moves = head_moves()
    tokens = img_emb.shape[0]
    half = tokens // 2
    rows = spec_emb.shape[0]
    second = lax.axis_index("co") == 1
    own = lax.all_gather(jnp.concatenate([spec_emb, grad_spec], axis=1), "co", tiled=True)
    own = jnp.concatenate(
        [jnp.where(second, a[:, SIZE:], a[:, :SIZE]) for a in (own[:, : 2 * SIZE], own[:, 2 * SIZE :])],
        axis=1,
    )
    own = lax.ppermute(own, EVERY, moves)
    features = 2 * img_emb.shape[1]
    image = jnp.concatenate([img_emb, grad_img], axis=1).T.reshape(features, 2, half)
    image = jnp.moveaxis(image, 1, 0)[None, :, None]
    image = jnp.broadcast_to(image, (2, 2, 8, features, half)).reshape(32, features, half)
    image = lax.all_to_all(image, GROUP, 0, 0, tiled=True)
    image = image.reshape(4, 8, 2, features // 2, half).transpose(2, 0, 3, 1, 4).reshape(2, SIZE, 8 * half)
    image_rows, image_grad = image[0], image[1]
    both = lax.all_gather(own, "co", tiled=True)
    spec_rows, spec_grad = both[:, :SIZE], both[:, SIZE:]

    across = ((1,), (0,))
    scores = dot(spec_rows, image_rows, across) * SCALE
    row_moment = dot(spec_grad, image_rows, across)
    column_moment = dot(spec_rows, image_grad, across)
    column_part, column_scaled = moments(scores, column_moment, 0)
    row_part, row_scaled = moments(scores, row_moment, 1)
    column_parts = lax.all_to_all(
        jnp.broadcast_to(column_part, (16, *column_part.shape)), ROWS, 0, 0, tiled=True
    )
    row_parts = lax.all_gather(row_part, "co")
    row_factor, row_delta = (t[:, None] for t in totals(row_parts, row_part))
    row_weight = row_scaled * row_factor
    row_slope = row_weight * (row_moment - row_delta)
    row_weight, row_slope = lax.optimization_barrier((row_weight.astype(jnp.bfloat16), row_slope))
    column_factor, column_delta = (t[None, :] for t in totals(column_parts, column_part))
    column_weight = column_scaled * column_factor
    slope = (row_slope + column_weight * (column_moment - column_delta)).astype(jnp.bfloat16)
    column_weight = column_weight.astype(jnp.bfloat16)
    last = ((1,), (1,))
    spec_part = SCALE * dot(image_rows, slope, last) + dot(image_grad, column_weight, last)
    first = ((0,), (0,))
    image_part = SCALE * dot(spec_rows, slope, first) + dot(spec_grad, row_weight, first)

    spec_parts = lax.all_gather(spec_part.astype(jnp.bfloat16), "co")
    spec_parts = jnp.where(second, spec_parts[:, :, 2 * rows :], spec_parts[:, :, : 2 * rows])
    spec_sum = (spec_parts[0].astype(jnp.float32) + spec_parts[1]).astype(jnp.bfloat16)
    spec_back = lax.ppermute(spec_sum, EVERY, [(b, a) for a, b in moves])

    image_part = image_part.astype(jnp.bfloat16).reshape(4, SIZE // 4, 8, half)
    image_part = jnp.moveaxis(image_part, 2, 1).reshape(32, SIZE // 4, half)
    image_parts = lax.all_to_all(image_part, GROUP, 0, 0, tiled=True)
    image_parts = image_parts.reshape(2, 2, 8, SIZE // 4, half).astype(jnp.float32)
    image_sum = jnp.sum(image_parts, axis=(0, 2)).astype(jnp.bfloat16)
    image_result = jnp.moveaxis(image_sum, 1, 2).reshape(tokens, SIZE // 4)

    spec_heads = lax.all_gather(spec_back, "co", tiled=True)
    spec_result = jnp.where(second, spec_heads[:, rows:], spec_heads[:, :rows]).T
    return (spec_result, image_result)


def solution(mesh):
    split = Mesh(mesh.devices.reshape((2,) * 9), EVERY)

    return jax.shard_map(
        shards,
        mesh=split,
        in_specs=(P(SPEC, IMG), P(IMG, SPEC), P(SPEC, IMG), P(IMG, SPEC)),
        out_specs=(P(SPEC, IMG), P(IMG, SPEC)),
        check_vma=False,
    )
```

```python
import jax
import jax.numpy as jnp
from jax import lax
from jax.experimental import pallas as pl
from jax.experimental.pallas import tpu as pltpu
from jax.sharding import Mesh
from jax.sharding import PartitionSpec as P


D = 1024
HEADS = 16
SIZE = D // HEADS
SPEC = ("xh", "z3", "z2", "z1", "z0", "co")
IMG = ("xl", "y1", "y0")
EVERY = SPEC + IMG
GROUP = ("z0", "co", "xl", "y1", "y0")
ROWS = ("z0", "xl", "y1", "y0")
SCALE = SIZE**-0.5


def head_moves():
    pairs = []
    for source in range(512):
        xh, z3, z2, z1, z0, co, xl, y1, y0 = ((source >> k) & 1 for k in range(8, -1, -1))
        target = 0
        for bit in (xl, y1, y0, co, z0 ^ z1 ^ co ^ 1, z1, xh, 1 - z3, 1 - z2):
            target = 2 * target + bit
        pairs.append((source, target))
    return pairs


def dot(a, b, dims):
    return lax.dot_general(a, b, (dims, ((), ())), preferred_element_type=jnp.float32)


BLOCK = 128
CHUNK = 16
LANES = 128


def row_blocks(total, size):
    return [slice(k, k + size) for k in range(0, total, size)]


def unpack(pieces, image):
    groups = image.shape[1] // LANES
    size = SIZE // 4
    for f in range(4):
        for k in range(groups):
            for kind in range(2):
                image[kind * SIZE + f * size : kind * SIZE + (f + 1) * size, k * LANES : (k + 1) * LANES] = (
                    pieces[f * groups + k, kind * size : (kind + 1) * size, :]
                )


def stats_kernel(both, pieces, column_out, row_out, z_ref, p_ref, q_ref, image):
    rows, tokens = z_ref.shape
    unpack(pieces, image)
    peak = None
    for block in row_blocks(rows, BLOCK):
        z = dot(both[block, :SIZE], image[:SIZE, :], ((1,), (0,))) * SCALE
        z_ref[block, :] = z
        q_ref[block, :] = dot(both[block, :SIZE], image[SIZE:, :], ((1,), (0,)))
        p_ref[block, :] = dot(both[block, SIZE:], image[:SIZE, :], ((1,), (0,)))
        for part in row_blocks(BLOCK, 8):
            peak = z[part] if peak is None else jnp.maximum(peak, z[part])
    high = jnp.max(peak, axis=0, keepdims=True)
    total = jnp.zeros((8, tokens), jnp.float32)
    weighted = jnp.zeros((8, tokens), jnp.float32)
    lane = lax.broadcasted_iota(jnp.int32, (8, LANES), 1)
    columns = []
    for part in row_blocks(rows, 8):
        z = z_ref[part, :]
        scaled = jnp.exp(z - high)
        total = total + scaled
        weighted = weighted + scaled * q_ref[part, :]
        row_high = jnp.max(z, axis=1, keepdims=True)
        scaled = jnp.exp(z - row_high)
        row_total = jnp.sum(scaled, axis=1, keepdims=True)
        row_weighted = jnp.sum(scaled * p_ref[part, :], axis=1, keepdims=True)
        columns.append(jnp.where(lane == 0, row_high, jnp.where(lane == 1, row_total, row_weighted)))
        if len(columns) * 8 == LANES:
            base = part.stop - LANES
            row_out[:, base : base + LANES] = jnp.concatenate(columns, axis=0).T[:8]
            columns = []
    sums = (
        high,
        jnp.sum(total, axis=0, keepdims=True),
        jnp.sum(weighted, axis=0, keepdims=True),
    )
    piece = jnp.concatenate([v[:, k] for v in sums for k in row_blocks(tokens, LANES)], axis=0)
    for peer in range(column_out.shape[0]):
        column_out[peer] = piece


def slope_kernel(
    both,
    turned,
    pieces,
    row_ref,
    column_ref,
    spec_out,
    image_out,
    z_ref,
    p_ref,
    q_ref,
    s_ref,
    r_ref,
    c_ref,
    image,
):
    rows, tokens = z_ref.shape
    unpack(pieces, image)
    groups = tokens // LANES
    across = ((1,), (0,))
    peers = column_ref.shape[0]
    high = column_ref[0, :groups]
    for peer in range(1, peers):
        high = jnp.maximum(high, column_ref[peer, :groups])
    total = weighted = 0.0
    for peer in range(peers):
        factor = jnp.exp(column_ref[peer, :groups] - high)
        total = total + column_ref[peer, groups : 2 * groups] * factor
        weighted = weighted + column_ref[peer, 2 * groups :] * factor
    shrink = 1.0 / total
    delta = weighted * shrink

    def products(block):
        z_ref[block, :] = dot(both[block, :SIZE], image[:SIZE, :], across) * SCALE
        p_ref[block, :] = dot(both[block, SIZE:], image[:SIZE, :], across)
        q_ref[block, :] = dot(both[block, :SIZE], image[SIZE:, :], across)

    blocks = row_blocks(rows, BLOCK)
    products(blocks[0])
    for n, block in enumerate(blocks):
        if n + 1 < len(blocks):
            products(blocks[n + 1])
        for part in row_blocks(BLOCK, CHUNK):
            part = slice(block.start + part.start, block.start + part.stop)
            row_high = jnp.broadcast_to(row_ref[part, 0:1], (CHUNK, LANES))
            row_shrink = jnp.broadcast_to(row_ref[part, 1:2], (CHUNK, LANES))
            row_delta = jnp.broadcast_to(row_ref[part, 2:3], (CHUNK, LANES))
            for k in range(groups):
                place = slice(k * LANES, (k + 1) * LANES)
                z = z_ref[part, place]
                row = jnp.exp(z - row_high) * row_shrink
                column = jnp.exp(z - high[k : k + 1]) * shrink[k : k + 1]
                slope = row * (p_ref[part, place] - row_delta) + column * (
                    q_ref[part, place] - delta[k : k + 1]
                )
                s_ref[part, place] = slope.astype(jnp.bfloat16)
                r_ref[part, place] = row.astype(jnp.bfloat16)
                c_ref[part, place] = column.astype(jnp.bfloat16)
        last = ((1,), (1,))
        spec_out[:, block] = (
            SCALE * dot(image[:SIZE, :], s_ref[block, :], last) + dot(image[SIZE:, :], c_ref[block, :], last)
        ).astype(jnp.bfloat16)
    image_part = SCALE * dot(turned[:SIZE, :], s_ref[...], across) + dot(turned[SIZE:, :], r_ref[...], across)
    image_part = image_part.astype(jnp.bfloat16)
    size = SIZE // 4
    for f in range(4):
        for k in range(groups):
            image_out[f * groups + k] = image_part[f * size : (f + 1) * size, k * LANES : (k + 1) * LANES]


def statistics(both, image, peers):
    rows, tokens = both.shape[0], image.shape[0] // 4 * LANES
    wide = pltpu.VMEM((rows, tokens), jnp.float32)
    return pl.pallas_call(
        stats_kernel,
        out_shape=(
            jax.ShapeDtypeStruct((peers, 3 * tokens // LANES, LANES), jnp.float32),
            jax.ShapeDtypeStruct((8, rows), jnp.float32),
        ),
        scratch_shapes=[wide, wide, wide, pltpu.VMEM((2 * SIZE, tokens), jnp.bfloat16)],
    )(both, image)


def gradients(both, turned, image, row_stats, column_parts):
    rows, tokens = both.shape[0], image.shape[0] // 4 * LANES
    wide = pltpu.VMEM((rows, tokens), jnp.float32)
    narrow = pltpu.VMEM((rows, tokens), jnp.bfloat16)
    return pl.pallas_call(
        slope_kernel,
        out_shape=(
            jax.ShapeDtypeStruct((SIZE, rows), jnp.bfloat16),
            jax.ShapeDtypeStruct((4 * tokens // LANES, SIZE // 4, LANES), jnp.bfloat16),
        ),
        scratch_shapes=[
            *(wide, wide, wide, narrow, narrow, narrow),
            pltpu.VMEM((2 * SIZE, tokens), jnp.bfloat16),
        ],
    )(both, turned, image, row_stats, column_parts)


def row_totals(parts):
    highest = jnp.max(parts[:, 0], axis=0)
    factor = jnp.exp(parts[:, 0] - highest)
    total = jnp.sum(parts[:, 1] * factor, axis=0)
    delta = jnp.sum(parts[:, 2] * factor, axis=0) / total
    return jnp.stack((highest, 1.0 / total, delta), axis=1)


def shards(spec_emb, img_emb, grad_spec, grad_img):
    moves = head_moves()
    tokens = img_emb.shape[0]
    half = tokens // 2
    rows = spec_emb.shape[0]
    second = lax.axis_index("co") == 1
    own = lax.all_gather(jnp.concatenate([spec_emb, grad_spec], axis=1), "co", tiled=True)
    own = jnp.concatenate(
        [jnp.where(second, a[:, SIZE:], a[:, :SIZE]) for a in (own[:, : 2 * SIZE], own[:, 2 * SIZE :])],
        axis=1,
    )
    own = lax.ppermute(own, EVERY, moves)
    features = 2 * img_emb.shape[1]
    image = jnp.concatenate([img_emb, grad_img], axis=1).T.reshape(features, 2, half)
    image = jnp.moveaxis(image, 1, 0)[None, :, None]
    image = jnp.broadcast_to(image, (2, 2, 8, features, half)).reshape(32, features, half)
    image = lax.all_to_all(image, GROUP, 0, 0, tiled=True)
    both = lax.all_gather(own, "co", tiled=True)
    column_part, row_part = statistics(both, image, 16)
    column_parts = lax.all_to_all(column_part, ROWS, 0, 0, tiled=True)
    row_parts = lax.all_gather(row_part, "co")
    row_stats = row_totals(row_parts)
    spec_part, image_part = gradients(both, both.T, image, row_stats, column_parts)
    spec_parts = lax.all_gather(spec_part, "co")
    spec_parts = jnp.where(second, spec_parts[:, :, 2 * rows :], spec_parts[:, :, : 2 * rows])
    spec_sum = (spec_parts[0].astype(jnp.float32) + spec_parts[1]).astype(jnp.bfloat16)
    spec_back = lax.ppermute(spec_sum, EVERY, [(b, a) for a, b in moves])

    image_parts = lax.all_to_all(image_part, GROUP, 0, 0, tiled=True)
    image_parts = image_parts.reshape(2, 2, 8, SIZE // 4, half).astype(jnp.float32)
    image_sum = jnp.sum(image_parts, axis=(0, 2)).astype(jnp.bfloat16)
    image_result = jnp.moveaxis(image_sum, 1, 2).reshape(tokens, SIZE // 4)

    spec_heads = lax.all_gather(spec_back, "co", tiled=True)
    spec_result = jnp.where(second, spec_heads[:, rows:], spec_heads[:, :rows]).T
    return (spec_result, image_result)


def solution(mesh):
    split = Mesh(mesh.devices.reshape((2,) * 9), EVERY)

    return jax.shard_map(
        shards,
        mesh=split,
        in_specs=(P(SPEC, IMG), P(IMG, SPEC), P(SPEC, IMG), P(IMG, SPEC)),
        out_specs=(P(SPEC, IMG), P(IMG, SPEC)),
        check_vma=False,
    )
```

```python
import jax
import jax.numpy as jnp
from jax import lax
from jax.experimental import pallas as pl
from jax.experimental.pallas import tpu as pltpu
from jax.sharding import Mesh
from jax.sharding import PartitionSpec as P


D = 1024
HEADS = 16
SIZE = D // HEADS
SPEC = ("xh", "z3", "z2", "z1", "z0", "co")
IMG = ("xl", "y1", "y0")
EVERY = SPEC + IMG
GROUP = ("z0", "co", "xl", "y1", "y0")
ROWS = ("z0", "xl", "y1", "y0")
SCALE = SIZE**-0.5


def head_moves():
    pairs = []
    for source in range(512):
        xh, z3, z2, z1, z0, co, xl, y1, y0 = ((source >> k) & 1 for k in range(8, -1, -1))
        target = 0
        for bit in (xl, y1, y0, co, z0 ^ z1 ^ co ^ 1, z1, xh, 1 - z3, z2):
            target = 2 * target + bit
        pairs.append((source, target))
    return pairs


def dot(a, b, dims):
    return lax.dot_general(a, b, (dims, ((), ())), preferred_element_type=jnp.float32)


BLOCK = 128
CHUNK = 16
LANES = 128
LIMIT = 20 * 2**20


def row_blocks(total, size):
    return [slice(k, k + size) for k in range(0, total, size)]


def unpack(pieces, image):
    groups = image.shape[1] // LANES
    size = SIZE // 4
    for f in range(4):
        for k in range(groups):
            for kind in range(2):
                image[kind * SIZE + f * size : kind * SIZE + (f + 1) * size, k * LANES : (k + 1) * LANES] = (
                    pieces[f * groups + k, kind * size : (kind + 1) * size, :]
                )


def stats_kernel(both, pieces, column_out, row_out, z_ref, p_ref, q_ref, image):
    rows, tokens = z_ref.shape
    unpack(pieces, image)
    peak = None
    for block in row_blocks(rows, BLOCK):
        z = dot(both[block, :SIZE], image[:SIZE, :], ((1,), (0,))) * SCALE
        z_ref[block, :] = z
        q_ref[block, :] = dot(both[block, :SIZE], image[SIZE:, :], ((1,), (0,)))
        p_ref[block, :] = dot(both[block, SIZE:], image[:SIZE, :], ((1,), (0,)))
        for part in row_blocks(BLOCK, 8):
            peak = z[part] if peak is None else jnp.maximum(peak, z[part])
    high = jnp.max(peak, axis=0, keepdims=True)
    total = jnp.zeros((8, tokens), jnp.float32)
    weighted = jnp.zeros((8, tokens), jnp.float32)
    lane = lax.broadcasted_iota(jnp.int32, (8, LANES), 1)
    columns = []
    for part in row_blocks(rows, 8):
        z = z_ref[part, :]
        scaled = jnp.exp(z - high)
        total = total + scaled
        weighted = weighted + scaled * q_ref[part, :]
        row_high = jnp.max(z, axis=1, keepdims=True)
        scaled = jnp.exp(z - row_high)
        row_total = jnp.sum(scaled, axis=1, keepdims=True)
        row_weighted = jnp.sum(scaled * p_ref[part, :], axis=1, keepdims=True)
        columns.append(jnp.where(lane == 0, row_high, jnp.where(lane == 1, row_total, row_weighted)))
        if len(columns) * 8 == LANES:
            base = part.stop - LANES
            row_out[:, base : base + LANES] = jnp.concatenate(columns, axis=0).T[:8]
            columns = []
    sums = (
        high,
        jnp.sum(total, axis=0, keepdims=True),
        jnp.sum(weighted, axis=0, keepdims=True),
    )
    piece = jnp.concatenate([v[:, k] for v in sums for k in row_blocks(tokens, LANES)], axis=0)
    for peer in range(column_out.shape[0]):
        column_out[peer] = piece


def slope_kernel(
    both,
    pieces,
    row_ref,
    column_ref,
    spec_out,
    image_out,
    z_ref,
    p_ref,
    q_ref,
    s_ref,
    r_ref,
    c_ref,
    image,
):
    rows, tokens = z_ref.shape
    unpack(pieces, image)
    groups = tokens // LANES
    across = ((1,), (0,))
    peers = column_ref.shape[0]
    high = column_ref[0, :groups]
    for peer in range(1, peers):
        high = jnp.maximum(high, column_ref[peer, :groups])
    total = weighted = 0.0
    for peer in range(peers):
        factor = jnp.exp(column_ref[peer, :groups] - high)
        total = total + column_ref[peer, groups : 2 * groups] * factor
        weighted = weighted + column_ref[peer, 2 * groups :] * factor
    shrink = 1.0 / total
    delta = weighted * shrink

    def products(block):
        z_ref[block, :] = dot(both[block, :SIZE], image[:SIZE, :], across) * SCALE
        p_ref[block, :] = dot(both[block, SIZE:], image[:SIZE, :], across)
        q_ref[block, :] = dot(both[block, :SIZE], image[SIZE:, :], across)

    blocks = row_blocks(rows, BLOCK)
    products(blocks[0])
    halves = []
    for n, block in enumerate(blocks):
        if n + 1 < len(blocks):
            products(blocks[n + 1])
        for part in row_blocks(BLOCK, CHUNK):
            part = slice(block.start + part.start, block.start + part.stop)
            row_high = jnp.broadcast_to(row_ref[part, 0:1], (CHUNK, LANES))
            row_shrink = jnp.broadcast_to(row_ref[part, 1:2], (CHUNK, LANES))
            row_delta = jnp.broadcast_to(row_ref[part, 2:3], (CHUNK, LANES))
            for k in range(groups):
                place = slice(k * LANES, (k + 1) * LANES)
                z = z_ref[part, place]
                row = jnp.exp(z - row_high) * row_shrink
                column = jnp.exp(z - high[k : k + 1]) * shrink[k : k + 1]
                slope = row * (p_ref[part, place] - row_delta) + column * (
                    q_ref[part, place] - delta[k : k + 1]
                )
                s_ref[part, place] = slope.astype(jnp.bfloat16)
                r_ref[part, place] = row.astype(jnp.bfloat16)
                c_ref[part, place] = column.astype(jnp.bfloat16)
        last = ((1,), (1,))
        part = SCALE * dot(s_ref[block, :], image[:SIZE, :], last)
        part = part + dot(c_ref[block, :], image[SIZE:, :], last)
        halves.append(part.astype(jnp.bfloat16))
        if len(halves) == 2:
            spec_out[n // 2] = jnp.concatenate(halves, axis=1)
            halves = []
    turned = both[...].astype(jnp.float32).T.astype(jnp.bfloat16)
    image_part = SCALE * dot(turned[:SIZE, :], s_ref[...], across) + dot(turned[SIZE:, :], r_ref[...], across)
    image_part = image_part.astype(jnp.bfloat16)
    size = SIZE // 4
    for f in range(4):
        for k in range(groups):
            image_out[f * groups + k] = image_part[f * size : (f + 1) * size, k * LANES : (k + 1) * LANES]


def statistics(both, image, peers):
    rows, tokens = both.shape[0], image.shape[0] // 4 * LANES
    wide = pltpu.VMEM((rows, tokens), jnp.float32)
    return pl.pallas_call(
        stats_kernel,
        out_shape=(
            jax.ShapeDtypeStruct((peers, 3 * tokens // LANES, LANES), jnp.float32),
            jax.ShapeDtypeStruct((8, rows), jnp.float32),
        ),
        compiler_params=pltpu.CompilerParams(vmem_limit_bytes=LIMIT),
        scratch_shapes=[wide, wide, wide, pltpu.VMEM((2 * SIZE, tokens), jnp.bfloat16)],
    )(both, image)


def gradients(both, image, row_stats, column_parts):
    rows, tokens = both.shape[0], image.shape[0] // 4 * LANES
    wide = pltpu.VMEM((rows, tokens), jnp.float32)
    narrow = pltpu.VMEM((rows, tokens), jnp.bfloat16)
    return pl.pallas_call(
        slope_kernel,
        out_shape=(
            jax.ShapeDtypeStruct((rows // (2 * BLOCK), BLOCK, 2 * SIZE), jnp.bfloat16),
            jax.ShapeDtypeStruct((4 * tokens // LANES, SIZE // 4, LANES), jnp.bfloat16),
        ),
        compiler_params=pltpu.CompilerParams(vmem_limit_bytes=LIMIT),
        scratch_shapes=[
            *(wide, wide, wide, narrow, narrow, narrow),
            pltpu.VMEM((2 * SIZE, tokens), jnp.bfloat16),
        ],
    )(both, image, row_stats, column_parts)


def row_totals(parts):
    highest = jnp.max(parts[:, 0], axis=0)
    factor = jnp.exp(parts[:, 0] - highest)
    total = jnp.sum(parts[:, 1] * factor, axis=0)
    delta = jnp.sum(parts[:, 2] * factor, axis=0) / total
    return jnp.stack((highest, 1.0 / total, delta), axis=1)


def shards(spec_emb, img_emb, grad_spec, grad_img):
    moves = head_moves()
    tokens = img_emb.shape[0]
    half = tokens // 2
    second = lax.axis_index("co") == 1
    own = lax.all_gather(jnp.concatenate([spec_emb, grad_spec], axis=1), "co", tiled=True)
    own = jnp.concatenate(
        [jnp.where(second, a[:, SIZE:], a[:, :SIZE]) for a in (own[:, : 2 * SIZE], own[:, 2 * SIZE :])],
        axis=1,
    )
    own = lax.ppermute(own, EVERY, moves)
    features = 2 * img_emb.shape[1]
    image = jnp.concatenate([img_emb, grad_img], axis=1).T.reshape(features, 2, half)
    image = jnp.moveaxis(image, 1, 0)[None, :, None]
    image = jnp.broadcast_to(image, (2, 2, 8, features, half)).reshape(32, features, half)
    image = lax.all_to_all(image, GROUP, 0, 0, tiled=True)
    both = lax.all_gather(own, "co", tiled=True)
    column_part, row_part = statistics(both, image, 16)
    column_parts = lax.all_to_all(column_part, ROWS, 0, 0, tiled=True)
    row_parts = lax.all_gather(row_part, "co")
    row_stats = row_totals(row_parts)
    spec_part, image_part = gradients(both, image, row_stats, column_parts)
    spec_parts = lax.all_gather(spec_part, "co")
    spec_parts = jnp.where(second, spec_parts[:, 1], spec_parts[:, 0])
    spec_sum = (spec_parts[0].astype(jnp.float32) + spec_parts[1]).astype(jnp.bfloat16)
    spec_back = lax.ppermute(spec_sum, EVERY, [(b, a) for a, b in moves])

    image_parts = lax.all_to_all(image_part, GROUP, 0, 0, tiled=True)
    image_parts = image_parts.reshape(2, 2, 8, SIZE // 4, half).astype(jnp.float32)
    image_sum = jnp.sum(image_parts, axis=(0, 2)).astype(jnp.bfloat16)
    image_result = jnp.moveaxis(image_sum, 1, 2).reshape(tokens, SIZE // 4)

    spec_heads = lax.all_gather(spec_back, "co")
    spec_heads = jnp.where(second, spec_heads[:, :, SIZE:], spec_heads[:, :, :SIZE])
    spec_result = jnp.concatenate([spec_heads[0], spec_heads[1]], axis=1)
    return (spec_result, image_result)


def solution(mesh):
    split = Mesh(mesh.devices.reshape((2,) * 9), EVERY)

    return jax.shard_map(
        shards,
        mesh=split,
        in_specs=(P(SPEC, IMG), P(IMG, SPEC), P(SPEC, IMG), P(IMG, SPEC)),
        out_specs=(P(SPEC, IMG), P(IMG, SPEC)),
        check_vma=False,
    )
```

```python
import jax
import jax.numpy as jnp
from jax import lax
from jax.experimental import pallas as pl
from jax.experimental.pallas import tpu as pltpu
from jax.sharding import Mesh
from jax.sharding import PartitionSpec as P


D = 1024
HEADS = 16
SIZE = D // HEADS
SPEC = ("xh", "z3", "z2", "z1", "z0", "co")
IMG = ("xl", "y1", "y0")
EVERY = SPEC + IMG
GROUP = ("z0", "co", "xl", "y1", "y0")
ROWS = ("z0", "xl", "y1", "y0")
SCALE = SIZE**-0.5


def head_moves():
    pairs = []
    for source in range(512):
        xh, z3, z2, z1, z0, co, xl, y1, y0 = ((source >> k) & 1 for k in range(8, -1, -1))
        target = 0
        for bit in (xl, y1, y0, co, z0 ^ z1 ^ co ^ 1, z1, xh, 1 - z3, z2):
            target = 2 * target + bit
        pairs.append((source, target))
    return pairs


def dot(a, b, dims):
    return lax.dot_general(a, b, (dims, ((), ())), preferred_element_type=jnp.float32)


BLOCK = 128
CHUNK = 16
LANES = 128
LIMIT = 20 * 2**20


def row_blocks(total, size):
    return [slice(k, k + size) for k in range(0, total, size)]


def unpack(pieces, image):
    groups = image.shape[1] // LANES
    size = SIZE // 4
    for f in range(4):
        for k in range(groups):
            for kind in range(2):
                image[kind * SIZE + f * size : kind * SIZE + (f + 1) * size, k * LANES : (k + 1) * LANES] = (
                    pieces[f * groups + k, kind * size : (kind + 1) * size, :]
                )


def stats_kernel(both, pieces, column_out, row_out, z_ref, p_ref, q_ref, image, piece_ref, sems):
    rows, tokens = z_ref.shape
    unpack(pieces, image)
    peak = None
    for block in row_blocks(rows, BLOCK):
        z = dot(both[block, :SIZE], image[:SIZE, :], ((1,), (0,))) * SCALE
        z_ref[block, :] = z
        q_ref[block, :] = dot(both[block, :SIZE], image[SIZE:, :], ((1,), (0,)))
        for part in row_blocks(BLOCK, 8):
            peak = z[part] if peak is None else jnp.maximum(peak, z[part])
    high = jnp.max(peak, axis=0, keepdims=True)
    total = jnp.zeros((8, tokens), jnp.float32)
    weighted = jnp.zeros((8, tokens), jnp.float32)
    for part in row_blocks(rows, 8):
        scaled = jnp.exp(z_ref[part, :] - high)
        total = total + scaled
        weighted = weighted + scaled * q_ref[part, :]
    sums = (
        high,
        jnp.sum(total, axis=0, keepdims=True),
        jnp.sum(weighted, axis=0, keepdims=True),
    )
    piece_ref[...] = jnp.concatenate([v[:, k] for v in sums for k in row_blocks(tokens, LANES)], axis=0)
    copies = [
        pltpu.make_async_copy(piece_ref, column_out.at[peer], sems.at[peer])
        for peer in range(column_out.shape[0])
    ]
    for copy in copies:
        copy.start()
    lane = lax.broadcasted_iota(jnp.int32, (8, LANES), 1)
    for block in row_blocks(rows, BLOCK):
        p_ref[block, :] = dot(both[block, SIZE:], image[:SIZE, :], ((1,), (0,)))
    for block in row_blocks(rows, LANES):
        columns = []
        for start in range(block.start, block.stop, 8):
            part = slice(start, start + 8)
            z = z_ref[part, :]
            row_high = jnp.max(z, axis=1, keepdims=True)
            scaled = jnp.exp(z - row_high)
            row_total = jnp.sum(scaled, axis=1, keepdims=True)
            row_weighted = jnp.sum(scaled * p_ref[part, :], axis=1, keepdims=True)
            columns.append(
                jnp.where(lane == 0, row_high, jnp.where(lane == 1, row_total, row_weighted))
            )
        row_out[:, block] = jnp.concatenate(columns, axis=0).T[:8]
    for copy in copies:
        copy.wait()


def row_kernel(both, pieces, row_ref, slope_out, image_out, z_ref, p_ref, r_ref, image):
    rows, tokens = z_ref.shape
    unpack(pieces, image)
    for block in row_blocks(rows, BLOCK):
        z_ref[block, :] = dot(both[block, :SIZE], image[:SIZE, :], ((1,), (0,))) * SCALE
        p_ref[block, :] = dot(both[block, SIZE:], image[:SIZE, :], ((1,), (0,)))
    for part in row_blocks(rows, CHUNK):
        row_high = jnp.broadcast_to(row_ref[part, 0:1], (CHUNK, LANES))
        row_shrink = jnp.broadcast_to(row_ref[part, 1:2], (CHUNK, LANES))
        row_delta = jnp.broadcast_to(row_ref[part, 2:3], (CHUNK, LANES))
        for place in row_blocks(tokens, LANES):
            row = jnp.exp(z_ref[part, place] - row_high) * row_shrink
            slope_out[part, place] = row * (p_ref[part, place] - row_delta)
            r_ref[part, place] = row.astype(jnp.bfloat16)
    turned = both[:, SIZE:].astype(jnp.float32).T.astype(jnp.bfloat16)
    image_out[...] = dot(turned, r_ref[...], ((1,), (0,)))


def slope_kernel(
    both, pieces, column_ref, row_slope, row_image, spec_out, image_out, z_ref, q_ref, s_ref, c_ref, image
):
    rows, tokens = z_ref.shape
    unpack(pieces, image)
    groups = tokens // LANES
    peers = column_ref.shape[0]
    high = column_ref[0, :groups]
    for peer in range(1, peers):
        high = jnp.maximum(high, column_ref[peer, :groups])
    total = weighted = 0.0
    for peer in range(peers):
        factor = jnp.exp(column_ref[peer, :groups] - high)
        total = total + column_ref[peer, groups : 2 * groups] * factor
        weighted = weighted + column_ref[peer, 2 * groups :] * factor
    shrink = 1.0 / total
    delta = weighted * shrink
    turned = both[:, :SIZE].astype(jnp.float32).T.astype(jnp.bfloat16)
    image_part = row_image[...]

    def products(block):
        z_ref[block, :] = dot(both[block, :SIZE], image[:SIZE, :], ((1,), (0,))) * SCALE
        q_ref[block, :] = dot(both[block, :SIZE], image[SIZE:, :], ((1,), (0,)))

    blocks = row_blocks(rows, BLOCK)
    products(blocks[0])
    halves = []
    for n, block in enumerate(blocks):
        if n + 1 < len(blocks):
            products(blocks[n + 1])
        for part in row_blocks(BLOCK, CHUNK):
            part = slice(block.start + part.start, block.start + part.stop)
            for k in range(groups):
                place = slice(k * LANES, (k + 1) * LANES)
                column = jnp.exp(z_ref[part, place] - high[k : k + 1]) * shrink[k : k + 1]
                slope = row_slope[part, place] + column * (q_ref[part, place] - delta[k : k + 1])
                s_ref[part, place] = slope.astype(jnp.bfloat16)
                c_ref[part, place] = column.astype(jnp.bfloat16)
        last = ((1,), (1,))
        part = SCALE * dot(s_ref[block, :], image[:SIZE, :], last)
        part = part + dot(c_ref[block, :], image[SIZE:, :], last)
        halves.append(part.astype(jnp.bfloat16))
        if len(halves) == 2:
            spec_out[n // 2] = jnp.concatenate(halves, axis=1)
            halves = []
    image_part = image_part + SCALE * dot(turned, s_ref[...], ((1,), (0,)))
    image_part = image_part.astype(jnp.bfloat16)
    size = SIZE // 4
    for f in range(4):
        for k in range(groups):
            image_out[f * groups + k] = image_part[f * size : (f + 1) * size, k * LANES : (k + 1) * LANES]


def statistics(both, pieces, peers):
    rows, tokens = both.shape[0], pieces.shape[0] // 4 * LANES
    wide = pltpu.VMEM((rows, tokens), jnp.float32)
    whole = pl.BlockSpec(memory_space=pltpu.VMEM)
    return pl.pallas_call(
        stats_kernel,
        out_shape=(
            jax.ShapeDtypeStruct((peers, 3 * tokens // LANES, LANES), jnp.float32),
            jax.ShapeDtypeStruct((8, rows), jnp.float32),
        ),
        in_specs=(whole, whole),
        out_specs=(pl.BlockSpec(memory_space=pl.ANY), whole),
        compiler_params=pltpu.CompilerParams(vmem_limit_bytes=LIMIT),
        scratch_shapes=[
            *(wide, wide, wide),
            pltpu.VMEM((2 * SIZE, tokens), jnp.bfloat16),
            pltpu.VMEM((3 * tokens // LANES, LANES), jnp.float32),
            pltpu.SemaphoreType.DMA((peers,)),
        ],
    )(both, pieces)


def row_side(both, pieces, row_stats):
    rows, tokens = both.shape[0], pieces.shape[0] // 4 * LANES
    wide = pltpu.VMEM((rows, tokens), jnp.float32)
    return pl.pallas_call(
        row_kernel,
        out_shape=(
            jax.ShapeDtypeStruct((rows, tokens), jnp.float32),
            jax.ShapeDtypeStruct((SIZE, tokens), jnp.float32),
        ),
        compiler_params=pltpu.CompilerParams(vmem_limit_bytes=LIMIT),
        scratch_shapes=[
            *(wide, wide),
            pltpu.VMEM((rows, tokens), jnp.bfloat16),
            pltpu.VMEM((2 * SIZE, tokens), jnp.bfloat16),
        ],
    )(both, pieces, row_stats)


def gradients(both, pieces, column_parts, row_slope, row_image):
    rows, tokens = row_slope.shape
    wide = pltpu.VMEM((rows, tokens), jnp.float32)
    narrow = pltpu.VMEM((rows, tokens), jnp.bfloat16)
    return pl.pallas_call(
        slope_kernel,
        out_shape=(
            jax.ShapeDtypeStruct((rows // (2 * BLOCK), BLOCK, 2 * SIZE), jnp.bfloat16),
            jax.ShapeDtypeStruct((4 * tokens // LANES, SIZE // 4, LANES), jnp.bfloat16),
        ),
        compiler_params=pltpu.CompilerParams(vmem_limit_bytes=LIMIT),
        scratch_shapes=[
            *(wide, wide, narrow, narrow),
            pltpu.VMEM((2 * SIZE, tokens), jnp.bfloat16),
        ],
    )(both, pieces, column_parts, row_slope, row_image)


def row_totals(parts):
    highest = jnp.max(parts[:, 0], axis=0)
    factor = jnp.exp(parts[:, 0] - highest)
    total = jnp.sum(parts[:, 1] * factor, axis=0)
    delta = jnp.sum(parts[:, 2] * factor, axis=0) / total
    return jnp.stack((highest, 1.0 / total, delta), axis=1)


def shards(spec_emb, img_emb, grad_spec, grad_img):
    moves = head_moves()
    tokens = img_emb.shape[0]
    half = tokens // 2
    second = lax.axis_index("co") == 1
    own = lax.all_gather(jnp.concatenate([spec_emb, grad_spec], axis=1), "co", tiled=True)
    own = jnp.concatenate(
        [jnp.where(second, a[:, SIZE:], a[:, :SIZE]) for a in (own[:, : 2 * SIZE], own[:, 2 * SIZE :])],
        axis=1,
    )
    own = lax.ppermute(own, EVERY, moves)
    features = 2 * img_emb.shape[1]
    image = jnp.concatenate([img_emb, grad_img], axis=1).T.reshape(features, 2, half)
    image = jnp.moveaxis(image, 1, 0)[None, :, None]
    image = jnp.broadcast_to(image, (2, 2, 8, features, half)).reshape(32, features, half)
    image = lax.all_to_all(image, GROUP, 0, 0, tiled=True)
    both = lax.all_gather(own, "co", tiled=True)
    column_part, row_part = statistics(both, image, 16)
    column_parts = lax.all_to_all(column_part, ROWS, 0, 0, tiled=True)
    row_parts = lax.all_gather(row_part, "co")
    row_stats = row_totals(row_parts)
    row_slope, row_image = row_side(both, image, row_stats)
    spec_part, image_part = gradients(both, image, column_parts, row_slope, row_image)
    spec_parts = lax.all_gather(spec_part, "co")
    spec_parts = jnp.where(second, spec_parts[:, 1], spec_parts[:, 0])
    spec_sum = (spec_parts[0].astype(jnp.float32) + spec_parts[1]).astype(jnp.bfloat16)
    spec_back = lax.ppermute(spec_sum, EVERY, [(b, a) for a, b in moves])

    image_parts = lax.all_to_all(image_part, GROUP, 0, 0, tiled=True)
    image_parts = image_parts.reshape(2, 2, 8, SIZE // 4, half).astype(jnp.float32)
    image_sum = jnp.sum(image_parts, axis=(0, 2)).astype(jnp.bfloat16)
    image_result = jnp.moveaxis(image_sum, 1, 2).reshape(tokens, SIZE // 4)

    spec_heads = lax.all_gather(spec_back, "co")
    spec_heads = jnp.where(second, spec_heads[:, :, SIZE:], spec_heads[:, :, :SIZE])
    spec_result = jnp.concatenate([spec_heads[0], spec_heads[1]], axis=1)
    return (spec_result, image_result)


def solution(mesh):
    split = Mesh(mesh.devices.reshape((2,) * 9), EVERY)

    return jax.shard_map(
        shards,
        mesh=split,
        in_specs=(P(SPEC, IMG), P(IMG, SPEC), P(SPEC, IMG), P(IMG, SPEC)),
        out_specs=(P(SPEC, IMG), P(IMG, SPEC)),
        check_vma=False,
    )
```

```python
import jax
import jax.numpy as jnp
from jax import lax
from jax.experimental import pallas as pl
from jax.experimental.pallas import tpu as pltpu
from jax.sharding import Mesh
from jax.sharding import PartitionSpec as P


D = 1024
HEADS = 16
SIZE = D // HEADS
SPEC = ("xh", "z3", "z2", "z1", "z0", "co")
IMG = ("xl", "y1", "y0")
EVERY = SPEC + IMG
GROUP = ("z0", "co", "xl", "y1", "y0")
ROWS = ("z0", "xl", "y1", "y0")
SCALE = SIZE**-0.5


def head_moves():
    pairs = []
    for source in range(512):
        xh, z3, z2, z1, z0, co, xl, y1, y0 = ((source >> k) & 1 for k in range(8, -1, -1))
        target = 0
        for bit in (xl, y1, y0, co, z0 ^ z1 ^ co ^ 1, z1, xh, 1 - z3, z2):
            target = 2 * target + bit
        pairs.append((source, target))
    return pairs


def dot(a, b, dims):
    return lax.dot_general(a, b, (dims, ((), ())), preferred_element_type=jnp.float32)


BLOCK = 128
CHUNK = 16
LANES = 128
LIMIT = 20 * 2**20


def row_blocks(total, size):
    return [slice(k, k + size) for k in range(0, total, size)]


def unpack(pieces, image):
    groups = image.shape[1] // LANES
    size = SIZE // 4
    for f in range(4):
        for k in range(groups):
            for kind in range(2):
                image[kind * SIZE + f * size : kind * SIZE + (f + 1) * size, k * LANES : (k + 1) * LANES] = (
                    pieces[f * groups + k, kind * size : (kind + 1) * size, :]
                )


def stats_kernel(both, pieces, column_out, row_out, z_ref, p_ref, q_ref, image, piece_ref, sems):
    rows, tokens = z_ref.shape
    unpack(pieces, image)
    peak = None
    for block in row_blocks(rows, BLOCK):
        z = dot(both[block, :SIZE], image[:SIZE, :], ((1,), (0,))) * SCALE
        z_ref[block, :] = z
        q_ref[block, :] = dot(both[block, :SIZE], image[SIZE:, :], ((1,), (0,)))
        for part in row_blocks(BLOCK, 8):
            peak = z[part] if peak is None else jnp.maximum(peak, z[part])
    high = jnp.max(peak, axis=0, keepdims=True)
    total = jnp.zeros((8, tokens), jnp.float32)
    weighted = jnp.zeros((8, tokens), jnp.float32)
    for part in row_blocks(rows, 8):
        scaled = jnp.exp(z_ref[part, :] - high)
        total = total + scaled
        weighted = weighted + scaled * q_ref[part, :]
    sums = (
        high,
        jnp.sum(total, axis=0, keepdims=True),
        jnp.sum(weighted, axis=0, keepdims=True),
    )
    piece_ref[...] = jnp.concatenate([v[:, k] for v in sums for k in row_blocks(tokens, LANES)], axis=0)
    copies = [
        pltpu.make_async_copy(piece_ref, column_out.at[peer], sems.at[peer])
        for peer in range(column_out.shape[0])
    ]
    for copy in copies:
        copy.start()
    lane = lax.broadcasted_iota(jnp.int32, (8, LANES), 1)
    for block in row_blocks(rows, BLOCK):
        p_ref[block, :] = dot(both[block, SIZE:], image[:SIZE, :], ((1,), (0,)))
    for block in row_blocks(rows, LANES):
        columns = []
        for start in range(block.start, block.stop, 8):
            part = slice(start, start + 8)
            z = z_ref[part, :]
            row_high = jnp.max(z, axis=1, keepdims=True)
            scaled = jnp.exp(z - row_high)
            row_total = jnp.sum(scaled, axis=1, keepdims=True)
            row_weighted = jnp.sum(scaled * p_ref[part, :], axis=1, keepdims=True)
            columns.append(
                jnp.where(lane == 0, row_high, jnp.where(lane == 1, row_total, row_weighted))
            )
        row_out[:, block] = jnp.concatenate(columns, axis=0).T[:8]
    for copy in copies:
        copy.wait()


def row_kernel(both, pieces, row_ref, slope_out, image_out, z_ref, p_ref, r_ref, image):
    rows, tokens = z_ref.shape
    unpack(pieces, image)
    for block in row_blocks(rows, BLOCK):
        z_ref[block, :] = dot(both[block, :SIZE], image[:SIZE, :], ((1,), (0,))) * SCALE
        p_ref[block, :] = dot(both[block, SIZE:], image[:SIZE, :], ((1,), (0,)))
    for part in row_blocks(rows, CHUNK):
        row_high = jnp.broadcast_to(row_ref[part, 0:1], (CHUNK, LANES))
        row_shrink = jnp.broadcast_to(row_ref[part, 1:2], (CHUNK, LANES))
        row_delta = jnp.broadcast_to(row_ref[part, 2:3], (CHUNK, LANES))
        for place in row_blocks(tokens, LANES):
            row = jnp.exp(z_ref[part, place] - row_high) * row_shrink
            slope_out[part, place] = row * (p_ref[part, place] - row_delta)
            r_ref[part, place] = row.astype(jnp.bfloat16)
    turned = both[:, SIZE:].astype(jnp.float32).T.astype(jnp.bfloat16)
    image_out[...] = dot(turned, r_ref[...], ((1,), (0,)))


def slope_kernel(
    both, pieces, column_ref, row_slope, row_image, spec_out, image_out, z_ref, q_ref, s_ref, c_ref, image
):
    rows, tokens = z_ref.shape
    unpack(pieces, image)
    groups = tokens // LANES
    peers = column_ref.shape[0]
    high = column_ref[0, :groups]
    for peer in range(1, peers):
        high = jnp.maximum(high, column_ref[peer, :groups])
    total = weighted = 0.0
    for peer in range(peers):
        factor = jnp.exp(column_ref[peer, :groups] - high)
        total = total + column_ref[peer, groups : 2 * groups] * factor
        weighted = weighted + column_ref[peer, 2 * groups :] * factor
    shrink = 1.0 / total
    delta = weighted * shrink
    turned = both[:, :SIZE].astype(jnp.float32).T.astype(jnp.bfloat16)
    image_part = row_image[...]

    def products(block):
        z_ref[block, :] = dot(both[block, :SIZE], image[:SIZE, :], ((1,), (0,))) * SCALE
        q_ref[block, :] = dot(both[block, :SIZE], image[SIZE:, :], ((1,), (0,)))

    blocks = row_blocks(rows, BLOCK)
    products(blocks[0])
    halves = []
    for n, block in enumerate(blocks):
        if n + 1 < len(blocks):
            products(blocks[n + 1])
        for part in row_blocks(BLOCK, CHUNK):
            part = slice(block.start + part.start, block.start + part.stop)
            for k in range(groups):
                place = slice(k * LANES, (k + 1) * LANES)
                column = jnp.exp(z_ref[part, place] - high[k : k + 1]) * shrink[k : k + 1]
                slope = row_slope[part, place] + column * (q_ref[part, place] - delta[k : k + 1])
                s_ref[part, place] = slope.astype(jnp.bfloat16)
                c_ref[part, place] = column.astype(jnp.bfloat16)
        last = ((1,), (1,))
        part = SCALE * dot(s_ref[block, :], image[:SIZE, :], last)
        part = part + dot(c_ref[block, :], image[SIZE:, :], last)
        halves.append(part.astype(jnp.bfloat16))
        if len(halves) == 2:
            spec_out[n // 2] = jnp.concatenate(halves, axis=1)
            halves = []
    image_part = image_part + SCALE * dot(turned, s_ref[...], ((1,), (0,)))
    image_part = image_part.astype(jnp.bfloat16)
    size = SIZE // 4
    for f in range(4):
        for k in range(groups):
            image_out[f * groups + k] = image_part[f * size : (f + 1) * size, k * LANES : (k + 1) * LANES]


def pack_kernel(spec_emb, grad_spec, image, grad, spec_out, pieces, image_ref, sems):
    width = spec_emb.shape[1]
    size = image.shape[0]
    count = pieces.shape[0]
    places = (
        (image, image_ref.at[:size]),
        (grad, image_ref.at[size:]),
        (spec_emb, spec_out.at[:, :width]),
        (grad_spec, spec_out.at[:, width:]),
    )
    copies = [pltpu.make_async_copy(a, b, sems.at[n]) for n, (a, b) in enumerate(places)]
    for copy in copies:
        copy.start()
    for copy in copies:
        copy.wait()
    for core in range(2):
        value = image_ref[:, core * LANES : (core + 1) * LANES]
        for k in range(count):
            if k // (count // 4) % 2 == core:
                pieces[k] = value


def packed(spec_emb, grad_spec, image, grad, peers):
    rows, width = spec_emb.shape
    size, tokens = image.shape
    return pl.pallas_call(
        pack_kernel,
        out_shape=(
            jax.ShapeDtypeStruct((rows, 2 * width), jnp.bfloat16),
            jax.ShapeDtypeStruct((peers, 2 * size, LANES), jnp.bfloat16),
        ),
        in_specs=(pl.BlockSpec(memory_space=pltpu.HBM),) * 4,
        compiler_params=pltpu.CompilerParams(vmem_limit_bytes=60 * 2**20),
        scratch_shapes=[
            pltpu.VMEM((2 * size, tokens), jnp.bfloat16),
            pltpu.SemaphoreType.DMA((4,)),
        ],
    )(spec_emb, grad_spec, image, grad)


def statistics(both, pieces, peers):
    rows, tokens = both.shape[0], pieces.shape[0] // 4 * LANES
    wide = pltpu.VMEM((rows, tokens), jnp.float32)
    whole = pl.BlockSpec(memory_space=pltpu.VMEM)
    return pl.pallas_call(
        stats_kernel,
        out_shape=(
            jax.ShapeDtypeStruct((peers, 3 * tokens // LANES, LANES), jnp.float32),
            jax.ShapeDtypeStruct((8, rows), jnp.float32),
        ),
        in_specs=(whole, whole),
        out_specs=(pl.BlockSpec(memory_space=pl.ANY), whole),
        compiler_params=pltpu.CompilerParams(vmem_limit_bytes=LIMIT),
        scratch_shapes=[
            *(wide, wide, wide),
            pltpu.VMEM((2 * SIZE, tokens), jnp.bfloat16),
            pltpu.VMEM((3 * tokens // LANES, LANES), jnp.float32),
            pltpu.SemaphoreType.DMA((peers,)),
        ],
    )(both, pieces)


def row_side(both, pieces, row_stats):
    rows, tokens = both.shape[0], pieces.shape[0] // 4 * LANES
    wide = pltpu.VMEM((rows, tokens), jnp.float32)
    return pl.pallas_call(
        row_kernel,
        out_shape=(
            jax.ShapeDtypeStruct((rows, tokens), jnp.float32),
            jax.ShapeDtypeStruct((SIZE, tokens), jnp.float32),
        ),
        compiler_params=pltpu.CompilerParams(vmem_limit_bytes=LIMIT),
        scratch_shapes=[
            *(wide, wide),
            pltpu.VMEM((rows, tokens), jnp.bfloat16),
            pltpu.VMEM((2 * SIZE, tokens), jnp.bfloat16),
        ],
    )(both, pieces, row_stats)


def gradients(both, pieces, column_parts, row_slope, row_image):
    rows, tokens = row_slope.shape
    wide = pltpu.VMEM((rows, tokens), jnp.float32)
    narrow = pltpu.VMEM((rows, tokens), jnp.bfloat16)
    return pl.pallas_call(
        slope_kernel,
        out_shape=(
            jax.ShapeDtypeStruct((rows // (2 * BLOCK), BLOCK, 2 * SIZE), jnp.bfloat16),
            jax.ShapeDtypeStruct((4 * tokens // LANES, SIZE // 4, LANES), jnp.bfloat16),
        ),
        compiler_params=pltpu.CompilerParams(vmem_limit_bytes=LIMIT),
        scratch_shapes=[
            *(wide, wide, narrow, narrow),
            pltpu.VMEM((2 * SIZE, tokens), jnp.bfloat16),
        ],
    )(both, pieces, column_parts, row_slope, row_image)


def row_totals(parts):
    highest = jnp.max(parts[:, 0], axis=0)
    factor = jnp.exp(parts[:, 0] - highest)
    total = jnp.sum(parts[:, 1] * factor, axis=0)
    delta = jnp.sum(parts[:, 2] * factor, axis=0) / total
    return jnp.stack((highest, 1.0 / total, delta), axis=1)


def shards(spec_emb, img_emb, grad_spec, grad_img):
    moves = head_moves()
    tokens = img_emb.shape[0]
    half = tokens // 2
    second = lax.axis_index("co") == 1
    own, image = packed(spec_emb, grad_spec, img_emb.T, grad_img.T, 32)
    image = lax.all_to_all(image, GROUP, 0, 0, tiled=True)
    own = lax.all_gather(own, "co", tiled=True)
    own = jnp.concatenate(
        [jnp.where(second, a[:, SIZE:], a[:, :SIZE]) for a in (own[:, : 2 * SIZE], own[:, 2 * SIZE :])],
        axis=1,
    )
    own = lax.ppermute(own, EVERY, moves)
    both = lax.all_gather(own, "co", tiled=True)
    column_part, row_part = statistics(both, image, 16)
    column_parts = lax.all_to_all(column_part, ROWS, 0, 0, tiled=True)
    row_parts = lax.all_gather(row_part, "co")
    row_stats = row_totals(row_parts)
    row_slope, row_image = row_side(both, image, row_stats)
    spec_part, image_part = gradients(both, image, column_parts, row_slope, row_image)
    spec_parts = lax.all_gather(spec_part, "co")
    spec_parts = jnp.where(second, spec_parts[:, 1], spec_parts[:, 0])
    spec_sum = (spec_parts[0].astype(jnp.float32) + spec_parts[1]).astype(jnp.bfloat16)
    spec_back = lax.ppermute(spec_sum, EVERY, [(b, a) for a, b in moves])

    image_parts = lax.all_to_all(image_part, GROUP, 0, 0, tiled=True)
    image_parts = image_parts.reshape(2, 2, 8, SIZE // 4, half).astype(jnp.float32)
    image_sum = jnp.sum(image_parts, axis=(0, 2)).astype(jnp.bfloat16)
    image_result = jnp.moveaxis(image_sum, 1, 2).reshape(tokens, SIZE // 4)

    spec_heads = lax.all_gather(spec_back, "co")
    spec_heads = jnp.where(second, spec_heads[:, :, SIZE:], spec_heads[:, :, :SIZE])
    spec_result = jnp.concatenate([spec_heads[0], spec_heads[1]], axis=1)
    return (spec_result, image_result)


def solution(mesh):
    split = Mesh(mesh.devices.reshape((2,) * 9), EVERY)

    return jax.shard_map(
        shards,
        mesh=split,
        in_specs=(P(SPEC, IMG), P(IMG, SPEC), P(SPEC, IMG), P(IMG, SPEC)),
        out_specs=(P(SPEC, IMG), P(IMG, SPEC)),
        check_vma=False,
    )
```
